32 devices in a mesh: seq: 32 (over z, y, x, core).
Axes of the slice: x: 2, y: 2, z: 4, core: 2. Of those that a mesh axis runs over, the one named last changes fastest.
Arguments:
- queries: bfloat16 [2, 8, 8192], replicated, may hold values from -4 to 4, as said below
- kv_pages: bfloat16 [8192, 4, 2, 1024], P('seq'), may hold values from -448 to 448
- page_scales: bfloat16 [8192, 32], P('seq'), may hold values from 0.39 to 4.02
- page_owner: int32 [8192], P('seq'), may hold values from 0 to 31, as said below
- valid_pages: int32 [32], P('seq'), may hold values from 192 to 256, as said below
- branch_kv: bfloat16 [2, 2, 8, 1024], replicated, may hold values from -128 to 128
- parents: int32 [8], replicated, may hold values from 0 to 7
Outputs:
- page_cache: bfloat16 [8192, 4, 2, 1024], P('seq')
- cache_scales: bfloat16 [8192, 32], P('seq')
- attended: float32 [2, 8, 8192], replicated
The draws below stay inside these ranges and needn't reach their ends.
Inputs may be any that keep to these rules, and one draw needn't show every extreme that they name: `queries`: within the range printed. page_owner[p] may be any device; at most 8 pages of one shard share an owner, and some shard sends 8 live pages to one owner; at most 256 live pages share an owner, and one owner has exactly 256. `valid_pages`: some shard has all 256 pages live.
All inputs are finite; a program needn't handle non-finite values.
Results may differ from the reference program's by a relative error of at most 0.001.
Values may be sent and summed in bfloat16 or wider, within the bound.
No kernel may reach another device: no remote copies, remote signals or barrier semaphores. Data moves between devices by JAX's collectives and lax.ppermute only.
A program may use at most 128 MiB of HBM per device.

```python
import math
import jax
import jax.numpy as jnp
from jax import lax

HQ = 64
KEY_VALUE_HEADS = 8
HEAD_SIZE = 128
LAYERS = 2
BEAMS = 8
PAGE = 2
P_DEV = 256
CAP = 8
WINDOW = 32
OWN_MAX = 256
PAGES = 8192
N_SEQ = 32


def base_queries(key):
    shape = (LAYERS, BEAMS, HQ, HEAD_SIZE)
    raw = jax.random.truncated_normal(jax.random.fold_in(key, 101), -4.0, 4.0, shape, jnp.float32)
    return raw.astype(jnp.bfloat16).astype(jnp.float32)


def base_scales(key):
    logs = jax.random.uniform(jax.random.fold_in(key, 111), (PAGES, 2 * LAYERS * KEY_VALUE_HEADS), jnp.float32, math.log(0.4), math.log(4.0))
    return jnp.exp(logs).astype(jnp.bfloat16).astype(jnp.float32)


def draw_queries(key, part):
    return base_queries(key).reshape(LAYERS, BEAMS, HQ * HEAD_SIZE).astype(jnp.bfloat16)


def draw_page_scales(key, part):
    return base_scales(key).astype(jnp.bfloat16)


def draw_kv_pages(key, part):
    shape = (PAGES, 2 * LAYERS, PAGE, KEY_VALUE_HEADS * HEAD_SIZE)
    entries = jax.random.truncated_normal(jax.random.fold_in(key, 121), -6.0, 6.0, shape, jnp.float32)
    return entries.astype(jnp.bfloat16)


def draw_branch_kv(key, part):
    queried = base_queries(key)
    centre = jnp.mean(queried.reshape(LAYERS, BEAMS, KEY_VALUE_HEADS, HQ // KEY_VALUE_HEADS, HEAD_SIZE), axis=(1, 3)).reshape(LAYERS, 1, KEY_VALUE_HEADS * HEAD_SIZE)
    shape = (LAYERS, BEAMS, KEY_VALUE_HEADS * HEAD_SIZE)
    noise_keys = jax.random.truncated_normal(jax.random.fold_in(key, 141), -6.0, 6.0, shape, jnp.float32)
    noise_values = jax.random.truncated_normal(jax.random.fold_in(key, 142), -6.0, 6.0, shape, jnp.float32)
    own_keys = 45.0 * centre + noise_keys
    stacked = jnp.stack([own_keys, noise_values], axis=1)
    return jnp.clip(stacked, -128.0, 128.0).astype(jnp.bfloat16)


def draw_valid_pages(key, part):
    counts = jax.random.randint(jax.random.fold_in(key, 131), (N_SEQ,), 3 * P_DEV // 4, P_DEV + 1)
    fullest = jax.random.randint(jax.random.fold_in(key, 132), (), 0, N_SEQ)
    return jnp.where(jnp.arange(N_SEQ, dtype=jnp.int32) == fullest, P_DEV, counts).astype(jnp.int32)


def draw_page_owner(key, part):
    live_least = 3 * P_DEV // 4
    lowest_count = (P_DEV + CAP - 1) // CAP
    busiest = jax.random.randint(jax.random.fold_in(key, 501), (), 0, N_SEQ)
    base_key = jax.random.fold_in(key, 502)
    reach_ids = jnp.arange(WINDOW, dtype=jnp.int32)
    reaches = jnp.where(reach_ids == 1, 1, reach_ids * N_SEQ // WINDOW).astype(jnp.int32)

    def one_shard(shard):
        shard_key = jax.random.fold_in(base_key, shard)
        noise = jax.random.randint(jax.random.fold_in(shard_key, 1), (WINDOW,), 0, 65536)
        positions = jnp.arange(WINDOW, dtype=jnp.int32)
        busiest_offset = (busiest - shard) % N_SEQ
        boost = jnp.where(reaches == busiest_offset, 1, 0)
        second = jnp.where(reaches == 1, 1, 0)
        score = boost * (65536 * WINDOW * 4) + second * (65536 * WINDOW * 2) + noise * WINDOW + positions
        order = jnp.argsort(-score, stable=True).astype(jnp.int32)
        kcount = jax.random.randint(jax.random.fold_in(shard_key, 2), (), lowest_count, WINDOW + 1)
        slot_ids = jnp.arange(P_DEV, dtype=jnp.int32)
        rest = 1 + (slot_ids - CAP) % jnp.maximum(kcount - 1, 1)
        slot_pick = jnp.where(slot_ids < CAP, 0, rest)
        slot_owner = (shard + reaches[order[slot_pick]]) % N_SEQ
        front = jax.random.permutation(jax.random.fold_in(shard_key, 3), live_least).astype(jnp.int32)
        back = live_least + jax.random.permutation(jax.random.fold_in(shard_key, 4), P_DEV - live_least).astype(jnp.int32)
        arranged = jnp.concatenate([front, back])
        return slot_owner[arranged]
    owners = jax.vmap(one_shard)(jnp.arange(N_SEQ, dtype=jnp.int32))
    return owners.reshape(PAGES).astype(jnp.int32)


def plant(drawn, own_key, smallest, top_value):
    longest = drawn.shape.index(max(drawn.shape))
    spots = []
    for shift in (0, 1):
        where = [jax.random.randint(jax.random.fold_in(own_key, axis), (), 0, length) for axis, length in enumerate(drawn.shape)]
        where[longest] = (where[longest] + shift) % drawn.shape[longest]
        spots.append(tuple(where))
    return drawn.at[spots[0]].set(smallest).at[spots[1]].set(top_value)


def setup_inputs(seed: int = 0) -> dict:
    key_list = jax.random.split(jax.random.key(seed), 8)
    return {
        "queries": draw_queries(jax.random.fold_in(key_list[7], 71), 0),
        "kv_pages": draw_kv_pages(jax.random.fold_in(key_list[7], 71), 0),
        "page_scales": draw_page_scales(jax.random.fold_in(key_list[7], 71), 0),
        "page_owner": draw_page_owner(jax.random.fold_in(key_list[7], 71), 0),
        "valid_pages": draw_valid_pages(jax.random.fold_in(key_list[7], 71), 0),
        "branch_kv": draw_branch_kv(jax.random.fold_in(key_list[7], 71), 0),
        "parents": plant(jax.random.randint(key_list[6], (BEAMS,), 0, BEAMS), jax.random.fold_in(key_list[6], 1), 0, BEAMS - 1).astype(jnp.int32),
    }


def reference(queries, kv_pages, page_scales, page_owner, valid_pages, branch_kv, parents):
    page_count = kv_pages.shape[0]
    per_shard = page_count // N_SEQ
    page_index = jnp.arange(page_count, dtype=jnp.int32)
    is_live = page_index % per_shard < valid_pages[page_index // per_shard]
    owner_hits = ((page_owner[:, None] == jnp.arange(N_SEQ, dtype=jnp.int32)[None, :]) & is_live[:, None]).astype(jnp.int32)
    rank_in = lax.optimization_barrier(jnp.sum((jnp.cumsum(owner_hits, axis=0) - 1) * owner_hits, axis=1))
    row_index = jnp.where(is_live, page_owner * OWN_MAX + rank_in, N_SEQ * OWN_MAX).astype(jnp.int32)
    page_cache = jnp.zeros((N_SEQ * OWN_MAX,) + kv_pages.shape[1:], kv_pages.dtype).at[row_index].set(kv_pages, mode='drop')
    cache_scales = jnp.zeros((N_SEQ * OWN_MAX, page_scales.shape[1]), page_scales.dtype).at[row_index].set(page_scales, mode='drop')
    group_size = HQ // KEY_VALUE_HEADS
    token_live = jnp.repeat(is_live, PAGE, total_repeat_length=page_count * PAGE)
    chooser = (parents[:, None] == jnp.arange(BEAMS, dtype=jnp.int32)[None, :]).astype(jnp.float32)
    results = []
    for current_layer_index in range(LAYERS):
        key_at = 2 * current_layer_index * KEY_VALUE_HEADS
        key_scale = page_scales[:, key_at:key_at + KEY_VALUE_HEADS].astype(jnp.float32)
        value_scale = page_scales[:, key_at + KEY_VALUE_HEADS:key_at + 2 * KEY_VALUE_HEADS].astype(jnp.float32)
        prompt_keys = (kv_pages[:, 2 * current_layer_index].astype(jnp.float32).reshape(page_count, PAGE, KEY_VALUE_HEADS, HEAD_SIZE) * key_scale[:, None, :, None]).reshape(page_count * PAGE, KEY_VALUE_HEADS, HEAD_SIZE)
        prompt_values = (kv_pages[:, 2 * current_layer_index + 1].astype(jnp.float32).reshape(page_count, PAGE, KEY_VALUE_HEADS, HEAD_SIZE) * value_scale[:, None, :, None]).reshape(page_count * PAGE, KEY_VALUE_HEADS, HEAD_SIZE)
        queried = queries[current_layer_index].astype(jnp.float32).reshape(BEAMS, KEY_VALUE_HEADS, group_size, HEAD_SIZE)
        own_keys = jnp.dot(chooser, branch_kv[current_layer_index, 0].astype(jnp.float32), precision=lax.Precision.HIGHEST).reshape(BEAMS, KEY_VALUE_HEADS, HEAD_SIZE)
        own_values = jnp.dot(chooser, branch_kv[current_layer_index, 1].astype(jnp.float32), precision=lax.Precision.HIGHEST).reshape(BEAMS, KEY_VALUE_HEADS, HEAD_SIZE)

        def head_group(packed):
            group_queries, group_keys, group_values, group_own_key, group_own_value = packed
            scores = jnp.einsum('brd,td->brt', group_queries, group_keys, precision=lax.Precision.HIGHEST) / math.sqrt(HEAD_SIZE)
            scores = jnp.where(token_live, scores, -jnp.inf)
            own_score = lax.optimization_barrier(jnp.sum(group_queries * group_own_key[:, None, :], axis=-1)) / math.sqrt(HEAD_SIZE)
            highest = jnp.maximum(lax.optimization_barrier(jnp.max(scores, axis=-1)), own_score)
            weights = jnp.exp(scores - highest[..., None])
            own_weight = jnp.exp(own_score - highest)
            totals = lax.optimization_barrier(jnp.sum(weights, axis=-1)) + own_weight
            mixture = jnp.einsum('brt,td->brd', weights, group_values, precision=lax.Precision.HIGHEST) + own_weight[..., None] * group_own_value[:, None, :]
            return mixture / totals[..., None]
        grouped = lax.map(head_group, (jnp.transpose(queried, (1, 0, 2, 3)), jnp.transpose(prompt_keys, (1, 0, 2)), jnp.transpose(prompt_values, (1, 0, 2)), jnp.transpose(own_keys, (1, 0, 2)), jnp.transpose(own_values, (1, 0, 2))))
        results.append(jnp.transpose(grouped, (1, 0, 2, 3)).reshape(BEAMS, HQ * HEAD_SIZE))
    return (page_cache, cache_scales, jnp.stack(results))
```

```python
import math

import jax
import jax.numpy as jnp
from jax import lax
from jax.experimental import pallas as pl
from jax.experimental.pallas import tpu as pltpu
from jax.sharding import PartitionSpec as P

HQ = 64
KEY_VALUE_HEADS = 8
HEAD_SIZE = 128
LAYERS = 2
BEAMS = 8
PAGE = 2
WAIT_PAGES = 32


def wait_pages(count, like_ref, sem):
    size = min(WAIT_PAGES, like_ref.shape[0])
    many, few = like_ref.at[pl.ds(0, size)], like_ref.at[0]

    def many_at_once(_, carry):
        pltpu.make_async_copy(many, many, sem).wait()
        return carry

    def one(_, carry):
        pltpu.make_async_copy(few, few, sem).wait()
        return carry

    lax.fori_loop(0, count // size, many_at_once, 0)
    lax.fori_loop(0, count % size, one, 0)


def pack_kernel(slot_count, owner_s, valid_s, owner_v, scales_t, pages, send_pages, send_scales, taken, sem):
    page_count = pages.shape[0]
    devices = taken.shape[0]
    live_count = valid_s[0]

    def clear(d, carry):
        taken[d] = 0
        return carry

    lax.fori_loop(0, devices, clear, 0)

    def send(p, carry):
        owner = owner_s[p]
        rank = taken[owner]
        taken[owner] = rank + 1
        pltpu.make_async_copy(pages.at[p], send_pages.at[owner * slot_count + rank], sem).start()
        return carry

    lax.fori_loop(0, live_count, send, 0)
    owners = owner_v[...]
    page_row = lax.broadcasted_iota(jnp.int32, (page_count, page_count), 0)
    page_col = lax.broadcasted_iota(jnp.int32, (page_count, page_count), 1)
    owner_row = jnp.broadcast_to(owners, (page_count, page_count))
    owner_col = jnp.transpose(owner_row)
    earlier = jnp.where((owner_row == owner_col) & (page_row < page_col), 1, 0)
    rank = jnp.sum(earlier, axis=0, keepdims=True)
    slot = jnp.where(page_col[:1] < live_count, owners * slot_count + rank, -1)
    slot_row = lax.broadcasted_iota(jnp.int32, (devices * slot_count, page_count), 0)
    chosen = jnp.where(slot_row == slot, 1.0, 0.0).astype(jnp.bfloat16)
    send_scales[...] = lax.dot_general(
        chosen, scales_t[...], (((1,), (1,)), ((), ())), preferred_element_type=jnp.float32
    ).astype(jnp.bfloat16)
    wait_pages(live_count, send_pages, sem)


def unpack_kernel(used_s, used_v, recv_scales, recv_pages, page_cache, cache_scales_t, zero_page, sem):
    slots = recv_pages.shape[0]
    own_max = page_cache.shape[0]
    zero_page[...] = jnp.zeros_like(zero_page)

    def keep(slot, row):
        is_used = used_s[slot]

        @pl.when(is_used > 0)
        def _():
            pltpu.make_async_copy(recv_pages.at[slot], page_cache.at[row], sem).start()

        return row + is_used

    total = lax.fori_loop(0, slots, keep, 0)

    def blank(row, carry):
        pltpu.make_async_copy(zero_page.at[0], page_cache.at[row], sem).start()
        return carry

    lax.fori_loop(total, own_max, blank, 0)
    used = used_v[...]
    slot_row = lax.broadcasted_iota(jnp.int32, (slots, slots), 0)
    slot_col = lax.broadcasted_iota(jnp.int32, (slots, slots), 1)
    used_col = jnp.transpose(jnp.broadcast_to(used, (slots, slots)))
    row = jnp.sum(jnp.where(slot_row < slot_col, used_col, 0), axis=0, keepdims=True)
    row = jnp.where(used > 0, row, -1)
    row_id = lax.broadcasted_iota(jnp.int32, (own_max, slots), 0)
    chosen = jnp.where(row_id == row, 1.0, 0.0).astype(jnp.bfloat16)
    cache_scales_t[...] = lax.dot_general(
        recv_scales[...], chosen, (((0,), (1,)), ((), ())), preferred_element_type=jnp.float32
    ).astype(jnp.bfloat16)
    wait_pages(own_max, page_cache, sem)


def pack(kv_pages, page_scales, page_owner, valid_pages, devices, slot_count):
    page_count, scale_count = page_scales.shape
    any_spec = pl.BlockSpec(memory_space=pl.ANY)
    smem = pl.BlockSpec(memory_space=pltpu.SMEM)
    vmem = pl.BlockSpec(memory_space=pltpu.VMEM)
    return pl.pallas_call(
        lambda *refs: pack_kernel(slot_count, *refs),
        out_shape=(
            jax.ShapeDtypeStruct((devices * slot_count,) + kv_pages.shape[1:], kv_pages.dtype),
            jax.ShapeDtypeStruct((devices * slot_count, scale_count), page_scales.dtype),
        ),
        in_specs=[smem, smem, vmem, vmem, any_spec],
        out_specs=(any_spec, vmem),
        scratch_shapes=[pltpu.SMEM((devices,), jnp.int32), pltpu.SemaphoreType.DMA],
        name="pack",
    )(page_owner, valid_pages, page_owner.reshape(1, page_count), page_scales.T, kv_pages)


def unpack(recv_pages, recv_scales, own_max):
    slots, scale_count = recv_scales.shape
    any_spec = pl.BlockSpec(memory_space=pl.ANY)
    smem = pl.BlockSpec(memory_space=pltpu.SMEM)
    vmem = pl.BlockSpec(memory_space=pltpu.VMEM)
    used = (recv_scales[:, 0] > 0).astype(jnp.int32)
    page_cache, cache_scales_t = pl.pallas_call(
        unpack_kernel,
        out_shape=(
            jax.ShapeDtypeStruct((own_max,) + recv_pages.shape[1:], recv_pages.dtype),
            jax.ShapeDtypeStruct((scale_count, own_max), recv_scales.dtype),
        ),
        in_specs=[smem, vmem, vmem, any_spec],
        out_specs=(any_spec, vmem),
        scratch_shapes=[pltpu.VMEM((1,) + recv_pages.shape[1:], recv_pages.dtype), pltpu.SemaphoreType.DMA],
        name="unpack",
    )(used, used.reshape(1, slots), recv_scales, recv_pages)
    return page_cache, cache_scales_t.T


def attend(queried, key_rows, value_rows, key_scale, value_scale, token_live):
    token_count = key_rows.shape[0] * PAGE
    keys = key_rows.reshape(token_count, KEY_VALUE_HEADS, HEAD_SIZE)
    values = value_rows.reshape(token_count, KEY_VALUE_HEADS, HEAD_SIZE)
    pages = key_rows.shape[0]

    def by_token(scale):
        spread = jnp.broadcast_to(scale.T[:, :, None].astype(jnp.float32), (KEY_VALUE_HEADS, pages, PAGE))
        return spread.reshape(KEY_VALUE_HEADS, token_count)

    scores = jnp.einsum("bgrd,tgd->gbrt", queried, keys, preferred_element_type=jnp.float32)
    scores = scores * (by_token(key_scale) / math.sqrt(HEAD_SIZE))[:, None, None, :]
    scores = jnp.where(token_live, scores, -1e30)
    maxima = jnp.max(scores, axis=-1)
    weights = jnp.where(token_live, jnp.exp(scores - maxima[..., None]), 0.0)
    totals = jnp.sum(weights, axis=-1)
    scaled = weights * by_token(value_scale)[:, None, None, :]
    high = lax.reduce_precision(scaled, 8, 7)
    low = (scaled - high).astype(jnp.bfloat16)
    mix = lambda part: jnp.einsum("gbrt,tgd->gbrd", part, values, preferred_element_type=jnp.float32)
    mixture = mix(high.astype(jnp.bfloat16)) + mix(low)
    return (jnp.moveaxis(maxima, 0, 1), jnp.moveaxis(totals, 0, 1), jnp.moveaxis(mixture, 0, 1))


def on_device(queries, kv_pages, page_scales, page_owner, valid_pages, branch_kv, parents):
    devices = lax.axis_size("seq")
    page_count = kv_pages.shape[0]
    slot_count = max(2, (page_count + devices - 1) // devices)
    own_max = slot_count * min(devices, page_count)
    group_size = HQ // KEY_VALUE_HEADS
    send_pages, send_scales = pack(kv_pages, page_scales, page_owner, valid_pages, devices, slot_count)
    recv_pages = lax.all_to_all(send_pages, "seq", split_axis=0, concat_axis=0, tiled=True)
    recv_scales = lax.all_to_all(send_scales, "seq", split_axis=0, concat_axis=0, tiled=True)
    page_cache, cache_scales = unpack(recv_pages, recv_scales, own_max)

    token_live = jnp.arange(page_count * PAGE, dtype=jnp.int32) < valid_pages[0] * PAGE
    queried = queries.reshape(LAYERS, BEAMS, KEY_VALUE_HEADS, group_size, HEAD_SIZE)
    partials = []
    for layer in range(LAYERS):
        key_at = 2 * layer * KEY_VALUE_HEADS
        partials.append(
            attend(
                queried[layer],
                kv_pages[:, 2 * layer],
                kv_pages[:, 2 * layer + 1],
                page_scales[:, key_at : key_at + KEY_VALUE_HEADS],
                page_scales[:, key_at + KEY_VALUE_HEADS : key_at + 2 * KEY_VALUE_HEADS],
                token_live,
            )
        )
    rows = LAYERS * BEAMS * HQ
    row_share = rows // devices
    maxima, totals, mixture = (jnp.stack([part[i] for part in partials]) for i in range(3))
    outgoing = jnp.concatenate(
        [
            mixture.reshape(devices, row_share * HEAD_SIZE),
            maxima.reshape(devices, row_share),
            totals.reshape(devices, row_share),
        ],
        axis=1,
    )
    incoming = lax.all_to_all(outgoing, "seq", split_axis=0, concat_axis=0, tiled=True)
    mixture = incoming[:, : row_share * HEAD_SIZE].reshape(devices, row_share, HEAD_SIZE)
    maxima = incoming[:, row_share * HEAD_SIZE : row_share * (HEAD_SIZE + 1)]
    totals = incoming[:, row_share * (HEAD_SIZE + 1) :]

    own_at = branch_kv[:, :, parents].astype(jnp.float32)
    own_key = own_at[:, 0].reshape(LAYERS, BEAMS, KEY_VALUE_HEADS, 1, HEAD_SIZE)
    own_value = own_at[:, 1].reshape(LAYERS, BEAMS, KEY_VALUE_HEADS, 1, HEAD_SIZE)
    own_score = jnp.sum(queried.astype(jnp.float32) * own_key, axis=-1) / math.sqrt(HEAD_SIZE)
    own_value = jnp.broadcast_to(own_value, (LAYERS, BEAMS, KEY_VALUE_HEADS, group_size, HEAD_SIZE))
    me = lax.axis_index("seq")
    own_score = lax.dynamic_slice(own_score.reshape(rows), (me * row_share,), (row_share,))
    own_value = lax.dynamic_slice(own_value.reshape(rows, HEAD_SIZE), (me * row_share, 0), (row_share, HEAD_SIZE))
    highest = jnp.maximum(jnp.max(maxima, axis=0), own_score)
    factor = jnp.exp(maxima - highest)
    own_factor = jnp.exp(own_score - highest)
    total = jnp.sum(totals * factor, axis=0) + own_factor
    mixed = jnp.sum(mixture * factor[..., None], axis=0) + own_factor[:, None] * own_value
    share = mixed / total[:, None]
    attended = lax.all_gather(share, "seq", axis=0, tiled=True)
    return (page_cache, cache_scales, attended.reshape(LAYERS, BEAMS, HQ * HEAD_SIZE))


def solution(mesh):
    return jax.shard_map(
        on_device,
        mesh=mesh,
        in_specs=(P(), P("seq", None, None, None), P("seq", None), P("seq"), P("seq"), P(), P()),
        out_specs=(P("seq", None, None, None), P("seq", None), P()),
        check_vma=False,
    )
```

```python
import math

import jax
import jax.numpy as jnp
from jax import lax
from jax.experimental import pallas as pl
from jax.experimental.pallas import tpu as pltpu
from jax.sharding import PartitionSpec as P


HQ = 64
KEY_VALUE_HEADS = 8
HEAD_SIZE = 128
LAYERS = 2
BEAMS = 8
PAGE = 2
WAIT_PAGES = 32
FETCH_CHUNKS = 4


def wait_pages(count, like_ref, sem):
    size = min(WAIT_PAGES, like_ref.shape[0])
    many, few = like_ref.at[pl.ds(0, size)], like_ref.at[0]

    def many_at_once(_, carry):
        pltpu.make_async_copy(many, many, sem).wait()
        return carry

    def one(_, carry):
        pltpu.make_async_copy(few, few, sem).wait()
        return carry

    lax.fori_loop(0, count // size, many_at_once, 0)
    lax.fori_loop(0, count % size, one, 0)


def pack_kernel(slot_count, owner_s, valid_s, owner_v, scales_t, pages, send_pages, send_scales, held, taken, sem, in_sems):
    page_count = pages.shape[0]
    devices = taken.shape[0]
    live_count = valid_s[0]
    chunks = in_sems.shape[0]
    size = page_count // chunks

    def fetch(c):
        part = pl.ds(c * size, size)
        return pltpu.make_async_copy(pages.at[part], held.at[part], in_sems.at[c])

    for c in range(chunks):
        fetch(c).start()

    def clear(d, carry):
        taken[d] = 0
        return carry

    lax.fori_loop(0, devices, clear, 0)

    def send(p, carry):
        owner = owner_s[p]
        rank = taken[owner]
        taken[owner] = rank + 1
        pltpu.make_async_copy(held.at[p], send_pages.at[owner * slot_count + rank], sem).start()
        return carry

    for c in range(chunks):
        fetch(c).wait()
        lax.fori_loop(c * size, jnp.clip(live_count, c * size, (c + 1) * size), send, 0)
    owners = owner_v[...]
    page_row = lax.broadcasted_iota(jnp.int32, (page_count, page_count), 0)
    page_col = lax.broadcasted_iota(jnp.int32, (page_count, page_count), 1)
    owner_row = jnp.broadcast_to(owners, (page_count, page_count))
    owner_col = jnp.transpose(owner_row)
    earlier = jnp.where((owner_row == owner_col) & (page_row < page_col), 1, 0)
    rank = jnp.sum(earlier, axis=0, keepdims=True)
    slot = jnp.where(page_col[:1] < live_count, owners * slot_count + rank, -1)
    slot_row = lax.broadcasted_iota(jnp.int32, (devices * slot_count, page_count), 0)
    chosen = jnp.where(slot_row == slot, 1.0, 0.0).astype(jnp.bfloat16)
    send_scales[...] = lax.dot_general(
        chosen, scales_t[...], (((1,), (1,)), ((), ())), preferred_element_type=jnp.float32
    ).astype(jnp.bfloat16)
    wait_pages(live_count, send_pages, sem)


def unpack_kernel(used_s, used_v, recv_scales, recv_pages, page_cache, cache_scales_t, held, zero_page, sem, in_sems):
    slots = recv_pages.shape[0]
    own_max = page_cache.shape[0]
    chunks = in_sems.shape[0]
    size = slots // chunks

    def fetch(c):
        part = pl.ds(c * size, size)
        return pltpu.make_async_copy(recv_pages.at[part], held.at[part], in_sems.at[c])

    for c in range(chunks):
        fetch(c).start()
    zero_page[...] = jnp.zeros_like(zero_page)

    def keep(slot, row):
        is_used = used_s[slot]

        @pl.when(is_used > 0)
        def _():
            pltpu.make_async_copy(held.at[slot], page_cache.at[row], sem).start()

        return row + is_used

    total = 0
    for c in range(chunks):
        fetch(c).wait()
        total = lax.fori_loop(c * size, (c + 1) * size, keep, total)

    def blank(row, carry):
        pltpu.make_async_copy(zero_page.at[0], page_cache.at[row], sem).start()
        return carry

    lax.fori_loop(total, own_max, blank, 0)
    used = used_v[...]
    slot_row = lax.broadcasted_iota(jnp.int32, (slots, slots), 0)
    slot_col = lax.broadcasted_iota(jnp.int32, (slots, slots), 1)
    used_col = jnp.transpose(jnp.broadcast_to(used, (slots, slots)))
    row = jnp.sum(jnp.where(slot_row < slot_col, used_col, 0), axis=0, keepdims=True)
    row = jnp.where(used > 0, row, -1)
    row_id = lax.broadcasted_iota(jnp.int32, (own_max, slots), 0)
    chosen = jnp.where(row_id == row, 1.0, 0.0).astype(jnp.bfloat16)
    cache_scales_t[...] = lax.dot_general(
        recv_scales[...], chosen, (((0,), (1,)), ((), ())), preferred_element_type=jnp.float32
    ).astype(jnp.bfloat16)
    wait_pages(own_max, page_cache, sem)


def fetch_chunks(pages):
    return math.gcd(FETCH_CHUNKS, pages)


def pack(kv_pages, page_scales, page_owner, valid_pages, devices, slot_count):
    page_count, scale_count = page_scales.shape
    any_spec = pl.BlockSpec(memory_space=pl.ANY)
    smem = pl.BlockSpec(memory_space=pltpu.SMEM)
    vmem = pl.BlockSpec(memory_space=pltpu.VMEM)
    return pl.pallas_call(
        lambda *refs: pack_kernel(slot_count, *refs),
        out_shape=(
            jax.ShapeDtypeStruct((devices * slot_count,) + kv_pages.shape[1:], kv_pages.dtype),
            jax.ShapeDtypeStruct((devices * slot_count, scale_count), page_scales.dtype),
        ),
        in_specs=[smem, smem, vmem, vmem, any_spec],
        out_specs=(any_spec, vmem),
        scratch_shapes=[
            pltpu.VMEM(kv_pages.shape, kv_pages.dtype),
            pltpu.SMEM((devices,), jnp.int32),
            pltpu.SemaphoreType.DMA,
            pltpu.SemaphoreType.DMA((fetch_chunks(page_count),)),
        ],
        name="pack",
    )(page_owner, valid_pages, page_owner.reshape(1, page_count), page_scales.T, kv_pages)


def unpack(recv_pages, recv_scales, own_max):
    slots, scale_count = recv_scales.shape
    any_spec = pl.BlockSpec(memory_space=pl.ANY)
    smem = pl.BlockSpec(memory_space=pltpu.SMEM)
    vmem = pl.BlockSpec(memory_space=pltpu.VMEM)
    used = (recv_scales[:, 0] > 0).astype(jnp.int32)
    page_cache, cache_scales_t = pl.pallas_call(
        unpack_kernel,
        out_shape=(
            jax.ShapeDtypeStruct((own_max,) + recv_pages.shape[1:], recv_pages.dtype),
            jax.ShapeDtypeStruct((scale_count, own_max), recv_scales.dtype),
        ),
        in_specs=[smem, vmem, vmem, any_spec],
        out_specs=(any_spec, vmem),
        scratch_shapes=[
            pltpu.VMEM(recv_pages.shape, recv_pages.dtype),
            pltpu.VMEM((1,) + recv_pages.shape[1:], recv_pages.dtype),
            pltpu.SemaphoreType.DMA,
            pltpu.SemaphoreType.DMA((fetch_chunks(slots),)),
        ],
        name="unpack",
    )(used, used.reshape(1, slots), recv_scales, recv_pages)
    return page_cache, cache_scales_t.T


def attend(queried, key_rows, value_rows, key_scale, value_scale, token_live):
    token_count = key_rows.shape[0] * PAGE
    keys = key_rows.reshape(token_count, KEY_VALUE_HEADS, HEAD_SIZE)
    values = value_rows.reshape(token_count, KEY_VALUE_HEADS, HEAD_SIZE)
    pages = key_rows.shape[0]

    def by_token(scale):
        spread = jnp.broadcast_to(scale.T[:, :, None].astype(jnp.float32), (KEY_VALUE_HEADS, pages, PAGE))
        return spread.reshape(KEY_VALUE_HEADS, token_count)

    scores = jnp.einsum("bgrd,tgd->gbrt", queried, keys, preferred_element_type=jnp.float32)
    scores = scores * (by_token(key_scale) / math.sqrt(HEAD_SIZE))[:, None, None, :]
    scores = jnp.where(token_live, scores, -1e30)
    maxima = jnp.max(scores, axis=-1)
    weights = jnp.where(token_live, jnp.exp(scores - maxima[..., None]), 0.0)
    totals = jnp.sum(weights, axis=-1)
    scaled = weights * by_token(value_scale)[:, None, None, :]
    high = lax.reduce_precision(scaled, 8, 7)
    low = (scaled - high).astype(jnp.bfloat16)
    mix = lambda part: jnp.einsum("gbrt,tgd->gbrd", part, values, preferred_element_type=jnp.float32)
    mixture = mix(high.astype(jnp.bfloat16)) + mix(low)
    return (jnp.moveaxis(maxima, 0, 1), jnp.moveaxis(totals, 0, 1), jnp.moveaxis(mixture, 0, 1))


def bits_of(devices):
    masks, mask = [], 1
    while mask < devices:
        masks.append(mask)
        mask *= 2
    return masks


def swap(array, mask, devices):
    return lax.ppermute(array, "seq", [(i, i ^ mask) for i in range(devices)])


def as_rows(values):
    count = -(-values.shape[0] // HEAD_SIZE)
    return jnp.pad(values, (0, count * HEAD_SIZE - values.shape[0])).reshape(count, HEAD_SIZE)


def reduce_step(state, blocks, axis, mask, is_high, devices):
    maxima, totals, mixture = state
    half = maxima.shape[0] // 2
    low, high = [part[:half] for part in state], [part[half:] for part in state]
    kept = [jnp.where(is_high, h, l) for l, h in zip(low, high)]
    sent = [jnp.where(is_high, l, h) for l, h in zip(low, high)]
    low_block, high_block = (lax.index_in_dim(blocks, i, axis, keepdims=False) for i in range(2))
    kept_block = jnp.where(is_high, high_block, low_block)
    sent_block = jnp.where(is_high, low_block, high_block)
    small = as_rows(jnp.concatenate([sent[0], sent[1]]))
    block_rows = sent_block.reshape(-1, HEAD_SIZE)
    received = swap(jnp.concatenate([sent[2], block_rows, small]), mask, devices)
    got_small = received[half + block_rows.shape[0] :].reshape(-1)
    got_block = received[half : half + block_rows.shape[0]].reshape(sent_block.shape)
    got_maxima, got_totals = got_small[:half], got_small[half : 2 * half]
    highest = jnp.maximum(kept[0], got_maxima)
    factor, got_factor = jnp.exp(kept[0] - highest), jnp.exp(got_maxima - highest)
    totals = kept[1] * factor + got_totals * got_factor
    mixture = kept[2] * factor[:, None] + received[:half] * got_factor[:, None]
    blocks = jnp.where(
        is_high, jnp.stack([got_block, kept_block], axis), jnp.stack([kept_block, got_block], axis)
    )
    return (highest, totals, mixture), blocks


def gather_step(rows, mask, is_high, devices):
    received = swap(rows, mask, devices)
    return jnp.where(is_high, jnp.concatenate([received, rows]), jnp.concatenate([rows, received]))


def on_device(queries, kv_pages, page_scales, page_owner, valid_pages, branch_kv, parents):
    devices = lax.axis_size("seq")
    page_count = kv_pages.shape[0]
    slot_count = max(2, (page_count + devices - 1) // devices)
    own_max = slot_count * min(devices, page_count)
    group_size = HQ // KEY_VALUE_HEADS
    send_pages, send_scales = pack(kv_pages, page_scales, page_owner, valid_pages, devices, slot_count)
    recv_pages = lax.all_to_all(send_pages, "seq", split_axis=0, concat_axis=0, tiled=True)

    token_live = jnp.arange(page_count * PAGE, dtype=jnp.int32) < valid_pages[0] * PAGE
    queried = queries.reshape(LAYERS, BEAMS, KEY_VALUE_HEADS, group_size, HEAD_SIZE)
    partials = []
    for layer in range(LAYERS):
        key_at = 2 * layer * KEY_VALUE_HEADS
        partials.append(
            attend(
                queried[layer],
                kv_pages[:, 2 * layer],
                kv_pages[:, 2 * layer + 1],
                page_scales[:, key_at : key_at + KEY_VALUE_HEADS],
                page_scales[:, key_at + KEY_VALUE_HEADS : key_at + 2 * KEY_VALUE_HEADS],
                token_live,
            )
        )
    rows = LAYERS * BEAMS * HQ
    maxima, totals, mixture = (jnp.stack([part[i] for part in partials]) for i in range(3))
    state = (maxima.reshape(rows), totals.reshape(rows), mixture.reshape(rows, HEAD_SIZE))
    me = lax.axis_index("seq")
    masks = bits_of(devices)
    block_size = slot_count * page_scales.shape[1]
    blocks = send_scales.astype(jnp.float32).reshape((2,) * len(masks) + (block_size,))
    for at, mask in enumerate(masks):
        state, blocks = reduce_step(state, blocks, len(masks) - 1 - at, mask, (me & mask) != 0, devices)
    recv_scales = blocks.reshape(devices * slot_count, page_scales.shape[1]).astype(page_scales.dtype)

    own_at = branch_kv[:, :, parents].astype(jnp.float32)
    own_key = own_at[:, 0].reshape(LAYERS, BEAMS, KEY_VALUE_HEADS, 1, HEAD_SIZE)
    own_value = own_at[:, 1].reshape(LAYERS, BEAMS, KEY_VALUE_HEADS, 1, HEAD_SIZE)
    own_score = jnp.sum(queried.astype(jnp.float32) * own_key, axis=-1) / math.sqrt(HEAD_SIZE)
    own_value = jnp.broadcast_to(own_value, (LAYERS, BEAMS, KEY_VALUE_HEADS, group_size, HEAD_SIZE))
    row_share = rows // devices
    order = sum(jnp.where((me & mask) != 0, devices // (2 * mask), 0) for mask in masks)
    first = order * row_share
    own_score = lax.dynamic_slice(own_score.reshape(rows), (first,), (row_share,))
    own_value = lax.dynamic_slice(own_value.reshape(rows, HEAD_SIZE), (first, 0), (row_share, HEAD_SIZE))
    maxima, totals, mixture = state
    highest = jnp.maximum(maxima, own_score)
    factor = jnp.exp(maxima - highest)
    own_factor = jnp.exp(own_score - highest)
    total = totals * factor + own_factor
    share = (mixture * factor[:, None] + own_factor[:, None] * own_value) / total[:, None]
    attended = share
    for mask in reversed(masks):
        attended = gather_step(attended, mask, (me & mask) != 0, devices)
    page_cache, cache_scales = unpack(recv_pages, recv_scales, own_max)
    return (page_cache, cache_scales, attended.reshape(LAYERS, BEAMS, HQ * HEAD_SIZE))


def solution(mesh):
    return jax.shard_map(
        on_device,
        mesh=mesh,
        in_specs=(P(), P("seq", None, None, None), P("seq", None), P("seq"), P("seq"), P(), P()),
        out_specs=(P("seq", None, None, None), P("seq", None), P()),
        check_vma=False,
    )
```

```python
import math

import jax
import jax.numpy as jnp
from jax import lax
from jax.experimental import pallas as pl
from jax.experimental.pallas import tpu as pltpu
from jax.sharding import PartitionSpec as P


HQ = 64
KEY_VALUE_HEADS = 8
HEAD_SIZE = 128
LAYERS = 2
BEAMS = 8
PAGE = 2
WAIT_PAGES = 32
MIB = 1 << 20
ISSUE = 8
CHUNKS = 4
FIRST_PART = 0.75


def wait_pages(count, like_ref, sem):
    size = min(WAIT_PAGES, like_ref.shape[0])
    many, few = like_ref.at[pl.ds(0, size)], like_ref.at[0]

    def many_at_once(_, carry):
        pltpu.make_async_copy(many, many, sem).wait()
        return carry

    def one(_, carry):
        pltpu.make_async_copy(few, few, sem).wait()
        return carry

    lax.fori_loop(0, count // size, many_at_once, 0)
    lax.fori_loop(0, count % size, one, 0)


def owner_ranks(owner_v):
    page_count = owner_v.shape[1]
    page_row = lax.broadcasted_iota(jnp.int32, (page_count, page_count), 0)
    page_col = lax.broadcasted_iota(jnp.int32, (page_count, page_count), 1)
    owner_row = jnp.broadcast_to(owner_v[...], (page_count, page_count))
    owner_col = jnp.transpose(owner_row)
    earlier = jnp.where((owner_row == owner_col) & (page_col < page_row), 1, 0)
    return owner_col[:, :1], jnp.sum(earlier, axis=1, keepdims=True)


def pack_pages(first_rank, slots, live_count, owner_v, pages, send, held, pages_v, pages_s, sem, in_sems, out_sem):
    page_count = pages.shape[0]
    total = send.shape[0]
    owner, rank = owner_ranks(owner_v)
    page_id = lax.broadcasted_iota(jnp.int32, (page_count, 1), 0)
    chosen = (page_id < live_count) & (rank >= first_rank) & (rank < first_rank + slots)
    place = jnp.where(chosen, owner * slots + rank - first_rank, -1)
    slot_id = lax.broadcasted_iota(jnp.int32, (page_count, total), 1)
    pages_v[...] = jnp.sum(jnp.where(place == slot_id, page_id, 0), axis=0, keepdims=True)
    to_scalars = pltpu.make_async_copy(pages_v, pages_s, sem)
    to_scalars.start()
    to_scalars.wait()
    chunks = in_sems.shape[0]
    size = total // chunks
    issue = math.gcd(size, ISSUE)
    for c in range(chunks):

        def fetch(step, carry):
            for i in range(issue):
                slot = c * size + step * issue + i
                pltpu.make_async_copy(pages.at[pages_s[0, slot]], held.at[slot], in_sems.at[c]).start()
            return carry

        lax.fori_loop(0, size // issue, fetch, 0)
    outs = []
    for c in range(chunks):
        part = pl.ds(c * size, size)
        pltpu.make_async_copy(held.at[part], held.at[part], in_sems.at[c]).wait()
        outs.append(pltpu.make_async_copy(held.at[part], send.at[part], out_sem.at[c]))
        outs[-1].start()
    for copy in outs:
        copy.wait()


def pack_first_kernel(slots, valid_s, owner_v, pages, send, *scratch):
    pack_pages(0, slots, valid_s[0], owner_v, pages, send, *scratch)


def pack_rest_kernel(first_slots, slot_count, valid_s, owner_v, scales_t, pages, send, send_scales, *scratch):
    page_count = pages.shape[0]
    slots = send_scales.shape[0]
    owner, rank = owner_ranks(owner_v)
    page_id = lax.broadcasted_iota(jnp.int32, (page_count, 1), 0)
    place = jnp.where(page_id < valid_s[0], owner * slot_count + rank, -1)
    slot_id = lax.broadcasted_iota(jnp.int32, (page_count, slots), 1)
    chosen = jnp.where(place == slot_id, 1.0, 0.0).astype(jnp.bfloat16)
    send_scales[...] = lax.dot_general(
        chosen, scales_t[...], (((0,), (1,)), ((), ())), preferred_element_type=jnp.float32
    )
    pack_pages(first_slots, slot_count - first_slots, valid_s[0], owner_v, pages, send, *scratch)


def unpack_first_kernel(counts_s, used_v, recv_scales, recv_pages, page_cache, cache_scales_t, zero_page, sem):
    own_max = page_cache.shape[0]
    slots = recv_scales.shape[0]
    devices = counts_s.shape[0]
    first_slots = recv_pages.shape[0] // devices
    zero_page[...] = jnp.zeros_like(zero_page)

    def keep(source, carry):
        row, copied = carry
        count = counts_s[source]

        def one(slot, inner):
            pltpu.make_async_copy(recv_pages.at[source * first_slots + slot], page_cache.at[row + slot], sem).start()
            return inner

        here = jnp.minimum(count, first_slots)
        lax.fori_loop(0, here, one, 0)
        return row + count, copied + here

    total, copied = lax.fori_loop(0, devices, keep, (0, 0))

    def blank(row, inner):
        pltpu.make_async_copy(zero_page.at[0], page_cache.at[row], sem).start()
        return inner

    lax.fori_loop(total, own_max, blank, 0)
    used = used_v[...]
    slot_row = lax.broadcasted_iota(jnp.int32, (slots, slots), 0)
    slot_col = lax.broadcasted_iota(jnp.int32, (slots, slots), 1)
    used_col = jnp.transpose(jnp.broadcast_to(used, (slots, slots)))
    row = jnp.sum(jnp.where(slot_row < slot_col, used_col, 0), axis=0, keepdims=True)
    row = jnp.where(used > 0, row, -1)
    row_id = lax.broadcasted_iota(jnp.int32, (own_max, slots), 0)
    chosen = jnp.where(row_id == row, 1.0, 0.0).astype(jnp.bfloat16)
    cache_scales_t[...] = lax.dot_general(
        recv_scales[...], chosen, (((0,), (1,)), ((), ())), preferred_element_type=jnp.float32
    ).astype(jnp.bfloat16)
    wait_pages(copied + own_max - total, page_cache, sem)


def unpack_rest_kernel(first_slots, counts_s, recv_pages, _, page_cache, held, sem, in_sems):
    devices = counts_s.shape[0]
    rest_slots = recv_pages.shape[0] // devices
    chunks = in_sems.shape[0]
    size = recv_pages.shape[0] // chunks
    parts = [pl.ds(c * size, size) for c in range(chunks)]
    fetches = [pltpu.make_async_copy(recv_pages.at[part], held.at[part], in_sems.at[c]) for c, part in enumerate(parts)]
    for fetch in fetches:
        fetch.start()

    def keep(source, carry):
        row, copied = carry
        count = counts_s[source]

        def one(slot, inner):
            pltpu.make_async_copy(
                held.at[source * rest_slots + slot], page_cache.at[row + first_slots + slot], sem
            ).start()
            return inner

        here = jnp.maximum(count - first_slots, 0)
        lax.fori_loop(0, here, one, 0)
        return row + count, copied + here

    carry = (0, 0)
    for c, fetch in enumerate(fetches):
        fetch.wait()
        carry = lax.fori_loop(c * size // rest_slots, (c + 1) * size // rest_slots, keep, carry)
    wait_pages(carry[1], page_cache, sem)


ANY = pl.BlockSpec(memory_space=pl.ANY)
SMEM = pl.BlockSpec(memory_space=pltpu.SMEM)
VMEM = pl.BlockSpec(memory_space=pltpu.VMEM)


def in_hbm(array):
    return pltpu.with_memory_space_constraint(array, pltpu.HBM)


def in_vmem(array):
    return pltpu.with_memory_space_constraint(array, pltpu.VMEM)


def pack_scratch(kv_pages, slots, chunks):
    return [
        pltpu.VMEM((slots,) + kv_pages.shape[1:], kv_pages.dtype),
        pltpu.VMEM((1, slots), jnp.int32),
        pltpu.SMEM((1, slots), jnp.int32),
        pltpu.SemaphoreType.DMA,
        pltpu.SemaphoreType.DMA((chunks,)),
        pltpu.SemaphoreType.DMA((chunks,)),
    ]


def pack_first(kv_pages, page_owner, valid_pages, devices, slots):
    page_count = kv_pages.shape[0]
    return pl.pallas_call(
        lambda *refs: pack_first_kernel(slots, *refs),
        out_shape=pltpu.HBM((devices * slots,) + kv_pages.shape[1:], kv_pages.dtype),
        in_specs=[SMEM, VMEM, ANY],
        out_specs=ANY,
        scratch_shapes=pack_scratch(kv_pages, devices * slots, math.gcd(CHUNKS, devices)),
        compiler_params=pltpu.CompilerParams(vmem_limit_bytes=8 * MIB),
        name="pack_first",
    )(valid_pages, page_owner.reshape(1, page_count), in_hbm(kv_pages))


def pack_rest(kv_pages, page_scales, page_owner, valid_pages, devices, slot_count, first_slots):
    page_count, scale_count = page_scales.shape
    slots = devices * (slot_count - first_slots)
    return pl.pallas_call(
        lambda *refs: pack_rest_kernel(first_slots, slot_count, *refs),
        out_shape=(
            pltpu.HBM((slots,) + kv_pages.shape[1:], kv_pages.dtype),
            pltpu.VMEM((devices * slot_count, scale_count), jnp.float32),
        ),
        in_specs=[SMEM, VMEM, VMEM, ANY],
        out_specs=(ANY, VMEM),
        scratch_shapes=pack_scratch(kv_pages, slots, math.gcd(CHUNKS, devices)),
        compiler_params=pltpu.CompilerParams(vmem_limit_bytes=8 * MIB),
        name="pack_rest",
    )(valid_pages, page_owner.reshape(1, page_count), page_scales.T, in_hbm(kv_pages))


def unpack_first(recv_pages, recv_scales, counts, own_max):
    slots, scale_count = recv_scales.shape
    used = (recv_scales[:, 0] > 0).astype(jnp.int32)
    return pl.pallas_call(
        lambda *refs: unpack_first_kernel(*refs),
        out_shape=(
            jax.ShapeDtypeStruct((own_max,) + recv_pages.shape[1:], recv_pages.dtype),
            jax.ShapeDtypeStruct((scale_count, own_max), recv_scales.dtype),
        ),
        in_specs=[SMEM, VMEM, VMEM, VMEM],
        out_specs=(ANY, VMEM),
        scratch_shapes=[
            pltpu.VMEM((1,) + recv_pages.shape[1:], recv_pages.dtype),
            pltpu.SemaphoreType.DMA,
        ],
        compiler_params=pltpu.CompilerParams(vmem_limit_bytes=4 * MIB),
        name="unpack_first",
    )(counts, used.reshape(1, slots), recv_scales, in_vmem(recv_pages))


def unpack_rest(recv_pages, counts, page_cache, first_slots):
    devices = counts.shape[0]
    return pl.pallas_call(
        lambda *refs: unpack_rest_kernel(first_slots, *refs),
        out_shape=jax.ShapeDtypeStruct(page_cache.shape, page_cache.dtype),
        in_specs=[SMEM, ANY, ANY],
        out_specs=ANY,
        input_output_aliases={2: 0},
        scratch_shapes=[
            pltpu.VMEM(recv_pages.shape, recv_pages.dtype),
            pltpu.SemaphoreType.DMA,
            pltpu.SemaphoreType.DMA((math.gcd(CHUNKS, devices),)),
        ],
        compiler_params=pltpu.CompilerParams(vmem_limit_bytes=4 * MIB),
        name="unpack_rest",
    )(counts, in_hbm(recv_pages), page_cache)


def as_row(column):
    return jnp.transpose(jnp.broadcast_to(column, (column.shape[0], HEAD_SIZE)))[:1]


def spread_rows(row):
    return jnp.transpose(jnp.broadcast_to(row, (HEAD_SIZE, row.shape[1])))


def small_count(share):
    return -(-2 * share // HEAD_SIZE)


def put_small(out, share, maxima, totals):
    both = jnp.concatenate([maxima, totals], axis=1)
    for at in range(small_count(share)):
        part = both[:, at * HEAD_SIZE : (at + 1) * HEAD_SIZE]
        out[share + at : share + at + 1, : part.shape[1]] = part


def get_small(rows, share):
    both = jnp.concatenate([rows[at : at + 1] for at in range(small_count(share))], axis=1)
    return both[:, :share], both[:, share : 2 * share]


def attend_kernel(units, place_s, valid_s, queries, scales_t, blocks, pages, *rest):
    outs, (token_scales, held, sems) = rest[:-3], rest[-3:]
    page_count = pages.shape[0]
    tokens = page_count * PAGE
    unit_rows = queries.shape[2]
    share = units * unit_rows
    groups, _, block_rows, _ = blocks.shape
    near = place_s[0]

    def unit_at(step, u):
        unit = (near ^ step) * units + u
        return unit // KEY_VALUE_HEADS, unit % KEY_VALUE_HEADS

    def fetch(step, u):
        layer, head = unit_at(step, u)
        lanes = pl.ds(pl.multiple_of(head * HEAD_SIZE, HEAD_SIZE), HEAD_SIZE)
        at = step * units + u
        return pltpu.make_async_copy(pages.at[:, pl.ds(2 * layer, 2), :, lanes], held.at[at], sems.at[at])

    order = [(step, u) for step in range(len(outs)) for u in range(units)]
    for step, u in order:
        fetch(step, u).start()
    page_id = lax.broadcasted_iota(jnp.int32, (page_count, tokens), 0)
    token_id = lax.broadcasted_iota(jnp.int32, (page_count, tokens), 1)
    spread = jnp.where(token_id // PAGE == page_id, 1.0, 0.0).astype(jnp.bfloat16)
    token_scales[...] = jnp.dot(scales_t[...], spread, preferred_element_type=jnp.float32)
    token_live = lax.broadcasted_iota(jnp.int32, (unit_rows, tokens), 1) < valid_s[0] * PAGE
    for step, out in enumerate(outs):
        maxima, totals = [], []
        for u in range(units):
            layer, head = unit_at(step, u)
            fetch(step, u).wait()
            keys = held[step * units + u, :, 0].reshape(tokens, HEAD_SIZE)
            values = held[step * units + u, :, 1].reshape(tokens, HEAD_SIZE)
            key_at = 2 * layer * KEY_VALUE_HEADS + head
            key_scale = token_scales[pl.ds(key_at, 1)] * (1 / math.sqrt(HEAD_SIZE))
            value_scale = token_scales[pl.ds(key_at + KEY_VALUE_HEADS, 1)]
            scores = lax.dot_general(
                queries[layer, head], keys, (((1,), (1,)), ((), ())), preferred_element_type=jnp.float32
            )
            scores = jnp.where(token_live, scores * key_scale, -1e30)
            highest = jnp.max(scores, axis=1, keepdims=True)
            weights = jnp.where(token_live, jnp.exp(scores - highest), 0.0)
            maxima.append(highest)
            totals.append(jnp.sum(weights, axis=1, keepdims=True))
            scaled = weights * value_scale
            high = scaled.astype(jnp.bfloat16)
            low = (scaled - high.astype(jnp.float32)).astype(jnp.bfloat16)
            mix = lambda part: jnp.dot(part, values, preferred_element_type=jnp.float32)
            out[u * unit_rows : (u + 1) * unit_rows] = mix(high) + mix(low)
        put_small(out, share, as_row(jnp.concatenate(maxima)), as_row(jnp.concatenate(totals)))
        for group in range(groups):
            at = share + small_count(share) + group * block_rows
            out[at : at + block_rows] = blocks[group, near ^ step]


def put_state(out, share, highest, total, mixture):
    out[:share] = mixture
    put_small(out, share, highest, total)


def put_blocks(payload, kept, first, entries, entry_at, size):
    for index in range(entries):
        payload[first + index * size : first + (index + 1) * size] = entry_at(0, index)
        kept[index * size : (index + 1) * size] = entry_at(1, index)


def merge_near_kernel(share, block_rows, groups, place_s, *refs):
    pieces, (payload, kept, sources) = refs[:-3], refs[-3:]
    near, far = place_s[0], place_s[1]
    first = share + small_count(share)
    smalls = [get_small(piece[share:first], share) for piece in pieces]
    highest = smalls[0][0]
    for maxima, _ in smalls[1:]:
        highest = jnp.maximum(highest, maxima)
    total, mixture = 0.0, 0.0
    for piece, (maxima, totals) in zip(pieces, smalls):
        factor = jnp.exp(maxima - highest)
        total += totals * factor
        mixture += piece[:share] * spread_rows(factor)
    put_state(payload, share, highest, total, mixture)
    for group in range(groups):
        for at, piece in enumerate(pieces):
            source = first + group * block_rows
            sources[group, pl.ds((near ^ at) * block_rows, block_rows)] = piece[source : source + block_rows]
    bit = far & 1

    def entry_at(mine, index):
        return sources[2 * index + (bit if mine else 1 - bit)]

    put_blocks(payload, kept, first, groups // 2, entry_at, sources.shape[1])


def far_merge(step, share, entry, place_s, own, kept, got, blocks):
    bit = (place_s[1] >> step) & 1
    first = share + small_count(share)
    entries = kept.shape[0] // entry
    width = 1 << step
    for index in range(entries):
        target, source = index // width, index % width
        at = target * 2 * width + source
        blocks[at + bit * width] = kept[index * entry : (index + 1) * entry]
        blocks[at + (1 - bit) * width] = got[first + index * entry : first + (index + 1) * entry]
    parts = []
    for rows, rows_other in ((own, got), (got, own)):
        pick = lambda at: jnp.where(bit == 0, rows[at], rows_other[at])
        maxima, totals = get_small(pick(slice(share, first)), share)
        parts.append((maxima, totals, pick(slice(0, share))))
    return parts


def merge_mid_kernel(step, share, entry, place_s, own, kept, got, payload, next_kept, blocks):
    (low_max, low_total, low_mix), (high_max, high_total, high_mix) = far_merge(
        step, share, entry, place_s, own, kept, got, blocks
    )
    highest = jnp.maximum(low_max, high_max)
    low, high = jnp.exp(low_max - highest), jnp.exp(high_max - highest)
    put_state(
        payload,
        share,
        highest,
        low_total * low + high_total * high,
        low_mix * spread_rows(low) + high_mix * spread_rows(high),
    )
    bit = (place_s[1] >> (step + 1)) & 1
    width = 2 << step

    def entry_at(mine, index):
        target, source = index // width, index % width
        return blocks[(2 * target + (bit if mine else 1 - bit)) * width + source]

    put_blocks(payload, next_kept, share + small_count(share), blocks.shape[0] // 2, entry_at, entry)


def merge_far_kernel(units, step, entry, place_s, parents_s, queries, branch, own, kept, got, out, out_blocks, blocks):
    near = place_s[0]
    unit_rows = queries.shape[2]
    share = units * unit_rows
    group_size = unit_rows // BEAMS
    states = far_merge(step, share, entry, place_s, own, kept, got, blocks)
    for index in range(blocks.shape[0]):
        out_blocks[index * entry : (index + 1) * entry] = blocks[index]
    beam_id = lax.broadcasted_iota(jnp.int32, (BEAMS, HEAD_SIZE), 0)
    own_scores, own_values = [], []
    for u in range(units):
        unit = near * units + u
        layer, head = unit // KEY_VALUE_HEADS, unit % KEY_VALUE_HEADS
        lanes = pl.ds(pl.multiple_of(head * HEAD_SIZE, HEAD_SIZE), HEAD_SIZE)
        keys, values = (branch[layer, kind, :, lanes].astype(jnp.float32) for kind in range(2))

        def chosen(rows):
            picked = [
                jnp.sum(jnp.where(beam_id == parents_s[beam], rows, 0.0), axis=0, keepdims=True)
                for beam in range(BEAMS)
            ]
            return jnp.concatenate([jnp.broadcast_to(row, (group_size, HEAD_SIZE)) for row in picked])

        own_scores.append(
            jnp.sum(queries[layer, head].astype(jnp.float32) * chosen(keys), axis=1, keepdims=True)
        )
        own_values.append(chosen(values))
    own_score = as_row(jnp.concatenate(own_scores)) / math.sqrt(HEAD_SIZE)
    highest = own_score
    for maxima, _, _ in states:
        highest = jnp.maximum(highest, maxima)
    factors = [jnp.exp(maxima - highest) for maxima, _, _ in states]
    own_factor = jnp.exp(own_score - highest)
    total = own_factor
    for (_, totals, _), factor in zip(states, factors):
        total += totals * factor
    mixture = jnp.concatenate(own_values) * spread_rows(own_factor / total)
    for (_, _, part), factor in zip(states, factors):
        mixture += part * spread_rows(factor / total)
    out[...] = mixture


def assemble_kernel(units, place_s, *refs):
    pieces, out = refs[:-1], refs[-1]
    unit_rows = pieces[0].shape[0] // units
    group_size = unit_rows // BEAMS
    for step, piece in enumerate(pieces):
        for u in range(units):
            unit = (place_s[0] ^ step) * units + u
            layer, head = unit // KEY_VALUE_HEADS, unit % KEY_VALUE_HEADS
            for query in range(group_size):
                at = pl.multiple_of((head * group_size + query) * HEAD_SIZE, HEAD_SIZE)
                out[layer, :, pl.ds(at, HEAD_SIZE)] = piece[pl.ds(u * unit_rows + query, BEAMS, stride=group_size)]


def partial_of(rows):
    return pltpu.VMEM((rows, HEAD_SIZE), jnp.float32)


def attend(place, queried, kv_pages, page_scales, valid_pages, blocks):
    page_count, scale_count = page_scales.shape
    groups, inner, block_rows, _ = blocks.shape
    units = LAYERS * KEY_VALUE_HEADS // inner
    share = units * queried.shape[2]
    return pl.pallas_call(
        lambda *refs: attend_kernel(units, *refs),
        in_specs=[SMEM, SMEM, VMEM, VMEM, VMEM, ANY],
        out_specs=(VMEM,) * inner,
        out_shape=(partial_of(share + small_count(share) + groups * block_rows),) * inner,
        scratch_shapes=[
            pltpu.VMEM((scale_count, page_count * PAGE), jnp.float32),
            pltpu.VMEM((inner * units, page_count, 2, PAGE, HEAD_SIZE), kv_pages.dtype),
            pltpu.SemaphoreType.DMA((inner * units,)),
        ],
        compiler_params=pltpu.CompilerParams(vmem_limit_bytes=12 * MIB),
        name="attend",
    )(place, valid_pages, queried, page_scales.T, blocks, in_hbm(kv_pages))


def far_shapes(share, entry, groups):
    return (
        partial_of(share + small_count(share) + groups // 2 * entry),
        partial_of(groups // 2 * entry),
    )


def merge_near(place, pieces, share, block_rows, groups):
    entry = len(pieces) * block_rows
    return pl.pallas_call(
        lambda *refs: merge_near_kernel(share, block_rows, groups, *refs),
        in_specs=[SMEM] + [VMEM] * len(pieces),
        out_specs=(VMEM, VMEM),
        out_shape=far_shapes(share, entry, groups),
        scratch_shapes=[pltpu.VMEM((groups, entry, HEAD_SIZE), jnp.float32)],
        compiler_params=pltpu.CompilerParams(vmem_limit_bytes=4 * MIB),
        name="merge_near",
    )(place, *map(in_vmem, pieces))


def merge_mid(place, step, own, kept, got, share, entry, groups):
    return pl.pallas_call(
        lambda *refs: merge_mid_kernel(step, share, entry, *refs),
        in_specs=[SMEM] + [VMEM] * 3,
        out_specs=(VMEM, VMEM),
        out_shape=far_shapes(share, entry, groups),
        scratch_shapes=[pltpu.VMEM((groups, entry, HEAD_SIZE), jnp.float32)],
        compiler_params=pltpu.CompilerParams(vmem_limit_bytes=4 * MIB),
        name="merge_mid",
    )(place, *map(in_vmem, (own, kept, got)))


def merge_far(place, step, parents, queried, branch_kv, own, kept, got, share, entry, groups):
    units = share // queried.shape[2]
    return pl.pallas_call(
        lambda *refs: merge_far_kernel(units, step, entry, *refs),
        in_specs=[SMEM, SMEM] + [VMEM] * 5,
        out_specs=(VMEM, VMEM),
        out_shape=(partial_of(share), partial_of(groups * entry)),
        scratch_shapes=[pltpu.VMEM((groups, entry, HEAD_SIZE), jnp.float32)],
        compiler_params=pltpu.CompilerParams(vmem_limit_bytes=4 * MIB),
        name="merge_far",
    )(place, parents, queried, branch_kv, *map(in_vmem, (own, kept, got)))


def assemble(place, pieces, units):
    return pl.pallas_call(
        lambda *refs: assemble_kernel(units, *refs),
        in_specs=[SMEM] + [VMEM] * len(pieces),
        out_specs=VMEM,
        out_shape=jax.ShapeDtypeStruct((LAYERS, BEAMS, HQ * HEAD_SIZE), jnp.float32),
        compiler_params=pltpu.CompilerParams(vmem_limit_bytes=4 * MIB),
        name="assemble",
    )(place, *map(in_vmem, pieces))


def bits_of(devices):
    masks, mask = [], 1
    while mask < devices:
        masks.append(mask)
        mask *= 2
    return masks


def swap(array, mask, devices):
    return lax.ppermute(array, "seq", [(i, i ^ mask) for i in range(devices)])


def exchange_pages(pages):
    return lax.all_to_all(pages, "seq", split_axis=0, concat_axis=0, tiled=True)


def on_device(queries, kv_pages, page_scales, page_owner, valid_pages, branch_kv, parents):
    devices = lax.axis_size("seq")
    page_count = kv_pages.shape[0]
    slot_count = max(2, (page_count + devices - 1) // devices)
    first_slots = max(1, int(slot_count * FIRST_PART))
    own_max = slot_count * min(devices, page_count)
    group_size = HQ // KEY_VALUE_HEADS
    rows = LAYERS * BEAMS * HQ
    send_first = pack_first(kv_pages, page_owner, valid_pages, devices, first_slots)
    send_rest, send_scales = pack_rest(kv_pages, page_scales, page_owner, valid_pages, devices, slot_count, first_slots)
    recv_first = exchange_pages(send_first)
    recv_rest = exchange_pages(send_rest)

    me = lax.axis_index("seq")
    masks = bits_of(devices)
    inner = 2 * masks[(len(masks) - 1) // 2]
    groups = devices // inner
    share = rows // inner
    place = jnp.stack([me % inner, me // inner]).astype(jnp.int32)
    block_size = slot_count * page_scales.shape[1]
    block_rows = -(-block_size // HEAD_SIZE)
    blocks = send_scales.reshape(devices, block_size)
    blocks = jnp.pad(blocks, ((0, 0), (0, block_rows * HEAD_SIZE - block_size)))
    blocks = blocks.reshape(groups, inner, block_rows, HEAD_SIZE)
    queried = queries.reshape(LAYERS, BEAMS, KEY_VALUE_HEADS, group_size, HEAD_SIZE).swapaxes(1, 2)
    queried = queried.reshape(LAYERS, KEY_VALUE_HEADS, BEAMS * group_size, HEAD_SIZE)
    pieces = attend(place, queried, kv_pages, page_scales, valid_pages, blocks)

    def spread(parts, masks):
        return [parts[0]] + [swap(part, mask, devices) for part, mask in zip(parts[1:], masks)]

    pieces = spread(pieces, range(1, inner))
    own, kept = merge_near(place, pieces, share, block_rows, groups)
    entry = inner * block_rows
    far_masks = [mask for mask in masks if mask >= inner]
    for step, mask in enumerate(far_masks):
        got = swap(own, mask, devices)
        if mask != far_masks[-1]:
            own, kept = merge_mid(place, step, own, kept, got, share, entry, groups)
    mine, blocks = merge_far(
        place, len(far_masks) - 1, parents, queried, branch_kv, own, kept, got, share, entry, groups
    )
    pieces = spread([mine] * inner, range(1, inner))
    attended = assemble(place, pieces, share // (BEAMS * group_size))
    blocks = blocks.reshape(devices, block_rows * HEAD_SIZE)[:, :block_size]
    recv_scales = blocks.reshape(devices * slot_count, page_scales.shape[1]).astype(page_scales.dtype)
    counts = jnp.sum((recv_scales[:, 0] > 0).astype(jnp.int32).reshape(devices, slot_count), axis=1)
    page_cache, cache_scales_t = unpack_first(recv_first, recv_scales, counts, own_max)
    page_cache = unpack_rest(recv_rest, counts, page_cache, first_slots)
    return (page_cache, cache_scales_t.T, attended)


def solution(mesh):
    return jax.shard_map(
        on_device,
        mesh=mesh,
        in_specs=(P(), P("seq", None, None, None), P("seq", None), P("seq"), P("seq"), P(), P()),
        out_specs=(P("seq", None, None, None), P("seq", None), P()),
        check_vma=False,
    )
```

```python
import math

import jax
import jax.numpy as jnp
from jax import lax
from jax.experimental import pallas as pl
from jax.experimental.pallas import tpu as pltpu
from jax.sharding import PartitionSpec as P


HQ = 64
KEY_VALUE_HEADS = 8
HEAD_SIZE = 128
LAYERS = 2
BEAMS = 8
PAGE = 2
WAIT_PAGES = 32
MIB = 1 << 20
ISSUE = 8
CHUNKS = 4
FIRST_PART = 0.75


def wait_pages(count, like_ref, sem):
    size = min(WAIT_PAGES, like_ref.shape[0])
    many, few = like_ref.at[pl.ds(0, size)], like_ref.at[0]

    def many_at_once(_, carry):
        pltpu.make_async_copy(many, many, sem).wait()
        return carry

    def one(_, carry):
        pltpu.make_async_copy(few, few, sem).wait()
        return carry

    lax.fori_loop(0, count // size, many_at_once, 0)
    lax.fori_loop(0, count % size, one, 0)


def owner_ranks(owner_v):
    page_count = owner_v.shape[1]
    page_row = lax.broadcasted_iota(jnp.int32, (page_count, page_count), 0)
    page_col = lax.broadcasted_iota(jnp.int32, (page_count, page_count), 1)
    owner_row = jnp.broadcast_to(owner_v[...], (page_count, page_count))
    owner_col = jnp.transpose(owner_row)
    earlier = jnp.where((owner_row == owner_col) & (page_col < page_row), 1, 0)
    return owner_col[:, :1], jnp.sum(earlier, axis=1, keepdims=True)


def pack_pages(first_rank, slots, live_count, owner_v, pages, send, held, pages_v, pages_s, sem, in_sems, out_sem):
    page_count = pages.shape[0]
    total = send.shape[0]
    owner, rank = owner_ranks(owner_v)
    page_id = lax.broadcasted_iota(jnp.int32, (page_count, 1), 0)
    chosen = (page_id < live_count) & (rank >= first_rank) & (rank < first_rank + slots)
    place = jnp.where(chosen, owner * slots + rank - first_rank, -1)
    slot_id = lax.broadcasted_iota(jnp.int32, (page_count, total), 1)
    pages_v[...] = jnp.sum(jnp.where(place == slot_id, page_id, 0), axis=0, keepdims=True)
    to_scalars = pltpu.make_async_copy(pages_v, pages_s, sem)
    to_scalars.start()
    to_scalars.wait()
    chunks = in_sems.shape[0]
    size = total // chunks
    issue = math.gcd(size, ISSUE)
    for c in range(chunks):

        def fetch(step, carry):
            for i in range(issue):
                slot = c * size + step * issue + i
                pltpu.make_async_copy(pages.at[pages_s[0, slot]], held.at[slot], in_sems.at[c]).start()
            return carry

        lax.fori_loop(0, size // issue, fetch, 0)
    outs = []
    for c in range(chunks):
        part = pl.ds(c * size, size)
        pltpu.make_async_copy(held.at[part], held.at[part], in_sems.at[c]).wait()
        outs.append(pltpu.make_async_copy(held.at[part], send.at[part], out_sem.at[c]))
        outs[-1].start()
    for copy in outs:
        copy.wait()


def pack_first_kernel(slots, valid_s, owner_v, pages, send, *scratch):
    pack_pages(0, slots, valid_s[0], owner_v, pages, send, *scratch)


def pack_rest_kernel(first_slots, slot_count, valid_s, owner_v, scales_t, pages, send, send_scales, *scratch):
    page_count = pages.shape[0]
    slots = send_scales.shape[0]
    owner, rank = owner_ranks(owner_v)
    page_id = lax.broadcasted_iota(jnp.int32, (page_count, 1), 0)
    place = jnp.where(page_id < valid_s[0], owner * slot_count + rank, -1)
    slot_id = lax.broadcasted_iota(jnp.int32, (page_count, slots), 1)
    chosen = jnp.where(place == slot_id, 1.0, 0.0).astype(jnp.bfloat16)
    send_scales[...] = lax.dot_general(
        chosen, scales_t[...], (((0,), (1,)), ((), ())), preferred_element_type=jnp.float32
    )
    pack_pages(first_slots, slot_count - first_slots, valid_s[0], owner_v, pages, send, *scratch)


def unpack_first_kernel(counts_s, used_v, recv_scales, recv_pages, page_cache, cache_scales_t, zero_page, sem):
    own_max = page_cache.shape[0]
    slots = recv_scales.shape[0]
    devices = counts_s.shape[0]
    first_slots = recv_pages.shape[0] // devices
    zero_page[...] = jnp.zeros_like(zero_page)

    def keep(source, carry):
        row, copied = carry
        count = counts_s[source]

        def one(slot, inner):
            pltpu.make_async_copy(recv_pages.at[source * first_slots + slot], page_cache.at[row + slot], sem).start()
            return inner

        here = jnp.minimum(count, first_slots)
        lax.fori_loop(0, here, one, 0)
        return row + count, copied + here

    total, copied = lax.fori_loop(0, devices, keep, (0, 0))

    def blank(row, inner):
        pltpu.make_async_copy(zero_page.at[0], page_cache.at[row], sem).start()
        return inner

    lax.fori_loop(total, own_max, blank, 0)
    used = used_v[...]
    slot_row = lax.broadcasted_iota(jnp.int32, (slots, slots), 0)
    slot_col = lax.broadcasted_iota(jnp.int32, (slots, slots), 1)
    used_col = jnp.transpose(jnp.broadcast_to(used, (slots, slots)))
    row = jnp.sum(jnp.where(slot_row < slot_col, used_col, 0), axis=0, keepdims=True)
    row = jnp.where(used > 0, row, -1)
    row_id = lax.broadcasted_iota(jnp.int32, (own_max, slots), 0)
    chosen = jnp.where(row_id == row, 1.0, 0.0).astype(jnp.bfloat16)
    cache_scales_t[...] = lax.dot_general(
        recv_scales[...], chosen, (((0,), (1,)), ((), ())), preferred_element_type=jnp.float32
    ).astype(jnp.bfloat16)
    wait_pages(copied + own_max - total, page_cache, sem)


def unpack_rest_kernel(first_slots, counts_s, recv_pages, _, page_cache, held, sem, in_sems):
    devices = counts_s.shape[0]
    rest_slots = recv_pages.shape[0] // devices
    chunks = in_sems.shape[0]
    size = recv_pages.shape[0] // chunks
    parts = [pl.ds(c * size, size) for c in range(chunks)]
    fetches = [pltpu.make_async_copy(recv_pages.at[part], held.at[part], in_sems.at[c]) for c, part in enumerate(parts)]
    for fetch in fetches:
        fetch.start()
    row, copied = 0, 0
    for c, fetch in enumerate(fetches):
        fetch.wait()
        for source in range(c * size // rest_slots, (c + 1) * size // rest_slots):
            count = counts_s[source]
            for slot in range(rest_slots):
                first = row + first_slots + slot

                @pl.when(count > first_slots + slot)
                def _():
                    pltpu.make_async_copy(held.at[source * rest_slots + slot], page_cache.at[first], sem).start()

            row += count
            copied += jnp.maximum(count - first_slots, 0)
    wait_pages(copied, page_cache, sem)


ANY = pl.BlockSpec(memory_space=pl.ANY)
SMEM = pl.BlockSpec(memory_space=pltpu.SMEM)
VMEM = pl.BlockSpec(memory_space=pltpu.VMEM)


def in_hbm(array):
    return pltpu.with_memory_space_constraint(array, pltpu.HBM)


def in_vmem(array):
    return pltpu.with_memory_space_constraint(array, pltpu.VMEM)


def pack_scratch(kv_pages, slots, chunks):
    return [
        pltpu.VMEM((slots,) + kv_pages.shape[1:], kv_pages.dtype),
        pltpu.VMEM((1, slots), jnp.int32),
        pltpu.SMEM((1, slots), jnp.int32),
        pltpu.SemaphoreType.DMA,
        pltpu.SemaphoreType.DMA((chunks,)),
        pltpu.SemaphoreType.DMA((chunks,)),
    ]


def pack_first(kv_pages, page_owner, valid_pages, devices, slots):
    page_count = kv_pages.shape[0]
    return pl.pallas_call(
        lambda *refs: pack_first_kernel(slots, *refs),
        out_shape=pltpu.HBM((devices * slots,) + kv_pages.shape[1:], kv_pages.dtype),
        in_specs=[SMEM, VMEM, ANY],
        out_specs=ANY,
        scratch_shapes=pack_scratch(kv_pages, devices * slots, math.gcd(CHUNKS, devices)),
        compiler_params=pltpu.CompilerParams(vmem_limit_bytes=8 * MIB),
        name="pack_first",
    )(valid_pages, page_owner.reshape(1, page_count), in_hbm(kv_pages))


def pack_rest(kv_pages, page_scales, page_owner, valid_pages, devices, slot_count, first_slots):
    page_count, scale_count = page_scales.shape
    slots = devices * (slot_count - first_slots)
    return pl.pallas_call(
        lambda *refs: pack_rest_kernel(first_slots, slot_count, *refs),
        out_shape=(
            pltpu.HBM((slots,) + kv_pages.shape[1:], kv_pages.dtype),
            pltpu.VMEM((devices * slot_count, scale_count), jnp.float32),
        ),
        in_specs=[SMEM, VMEM, VMEM, ANY],
        out_specs=(ANY, VMEM),
        scratch_shapes=pack_scratch(kv_pages, slots, math.gcd(CHUNKS, devices)),
        compiler_params=pltpu.CompilerParams(vmem_limit_bytes=8 * MIB),
        name="pack_rest",
    )(valid_pages, page_owner.reshape(1, page_count), page_scales.T, in_hbm(kv_pages))


def unpack_first(recv_pages, recv_scales, counts, own_max):
    slots, scale_count = recv_scales.shape
    used = (recv_scales[:, 0] > 0).astype(jnp.int32)
    return pl.pallas_call(
        lambda *refs: unpack_first_kernel(*refs),
        out_shape=(
            jax.ShapeDtypeStruct((own_max,) + recv_pages.shape[1:], recv_pages.dtype),
            jax.ShapeDtypeStruct((scale_count, own_max), recv_scales.dtype),
        ),
        in_specs=[SMEM, VMEM, VMEM, VMEM],
        out_specs=(ANY, VMEM),
        scratch_shapes=[
            pltpu.VMEM((1,) + recv_pages.shape[1:], recv_pages.dtype),
            pltpu.SemaphoreType.DMA,
        ],
        compiler_params=pltpu.CompilerParams(vmem_limit_bytes=4 * MIB),
        name="unpack_first",
    )(counts, used.reshape(1, slots), recv_scales, recv_pages)


def unpack_rest(recv_pages, counts, page_cache, first_slots):
    devices = counts.shape[0]
    return pl.pallas_call(
        lambda *refs: unpack_rest_kernel(first_slots, *refs),
        out_shape=jax.ShapeDtypeStruct(page_cache.shape, page_cache.dtype),
        in_specs=[SMEM, ANY, ANY],
        out_specs=ANY,
        input_output_aliases={2: 0},
        scratch_shapes=[
            pltpu.VMEM(recv_pages.shape, recv_pages.dtype),
            pltpu.SemaphoreType.DMA,
            pltpu.SemaphoreType.DMA((math.gcd(CHUNKS, devices),)),
        ],
        compiler_params=pltpu.CompilerParams(vmem_limit_bytes=4 * MIB),
        name="unpack_rest",
    )(counts, in_hbm(recv_pages), page_cache)


def as_row(column):
    return jnp.transpose(jnp.broadcast_to(column, (column.shape[0], HEAD_SIZE)))[:1]


def spread_rows(row):
    return jnp.transpose(jnp.broadcast_to(row, (HEAD_SIZE, row.shape[1])))


def small_count(share):
    return -(-2 * share // HEAD_SIZE)


def put_small(out, share, maxima, totals):
    both = jnp.concatenate([maxima, totals], axis=1)
    for at in range(small_count(share)):
        part = both[:, at * HEAD_SIZE : (at + 1) * HEAD_SIZE]
        out[share + at : share + at + 1, : part.shape[1]] = part


def get_small(rows, share):
    both = jnp.concatenate([rows[at : at + 1] for at in range(small_count(share))], axis=1)
    return both[:, :share], both[:, share : 2 * share]


def attend_kernel(units, place_s, valid_s, queries, scales_t, blocks, pages, *rest):
    outs, (token_scales, held, sems) = rest[:-3], rest[-3:]
    page_count = pages.shape[0]
    tokens = page_count * PAGE
    unit_rows = queries.shape[2]
    share = units * unit_rows
    groups, _, block_rows, _ = blocks.shape
    near = place_s[0]

    def unit_at(step, u):
        unit = (near ^ step) * units + u
        return unit // KEY_VALUE_HEADS, unit % KEY_VALUE_HEADS

    def fetch(step, u):
        layer, head = unit_at(step, u)
        lanes = pl.ds(pl.multiple_of(head * HEAD_SIZE, HEAD_SIZE), HEAD_SIZE)
        at = step * units + u
        return pltpu.make_async_copy(pages.at[:, pl.ds(2 * layer, 2), :, lanes], held.at[at], sems.at[at])

    order = [(step, u) for step in range(len(outs)) for u in range(units)]
    for step, u in order:
        fetch(step, u).start()
    page_id = lax.broadcasted_iota(jnp.int32, (page_count, tokens), 0)
    token_id = lax.broadcasted_iota(jnp.int32, (page_count, tokens), 1)
    spread = jnp.where(token_id // PAGE == page_id, 1.0, 0.0).astype(jnp.bfloat16)
    token_scales[...] = jnp.dot(scales_t[...], spread, preferred_element_type=jnp.float32)
    token_live = lax.broadcasted_iota(jnp.int32, (unit_rows, tokens), 1) < valid_s[0] * PAGE
    for step, out in enumerate(outs):
        maxima, totals = [], []
        for u in range(units):
            layer, head = unit_at(step, u)
            fetch(step, u).wait()
            keys = held[step * units + u, :, 0].reshape(tokens, HEAD_SIZE)
            values = held[step * units + u, :, 1].reshape(tokens, HEAD_SIZE)
            key_at = 2 * layer * KEY_VALUE_HEADS + head
            key_scale = token_scales[pl.ds(key_at, 1)] * (1 / math.sqrt(HEAD_SIZE))
            value_scale = token_scales[pl.ds(key_at + KEY_VALUE_HEADS, 1)]
            scores = lax.dot_general(
                queries[layer, head], keys, (((1,), (1,)), ((), ())), preferred_element_type=jnp.float32
            )
            scores = jnp.where(token_live, scores * key_scale, -1e30)
            highest = jnp.max(scores, axis=1, keepdims=True)
            weights = jnp.where(token_live, jnp.exp(scores - highest), 0.0)
            maxima.append(highest)
            totals.append(jnp.sum(weights, axis=1, keepdims=True))
            scaled = weights * value_scale
            high = scaled.astype(jnp.bfloat16)
            low = (scaled - high.astype(jnp.float32)).astype(jnp.bfloat16)
            mix = lambda part: jnp.dot(part, values, preferred_element_type=jnp.float32)
            out[u * unit_rows : (u + 1) * unit_rows] = mix(high) + mix(low)
        put_small(out, share, as_row(jnp.concatenate(maxima)), as_row(jnp.concatenate(totals)))
        for group in range(groups):
            at = share + small_count(share) + group * block_rows
            out[at : at + block_rows] = blocks[group, near ^ step]


def put_state(out, share, highest, total, mixture):
    out[:share] = mixture
    put_small(out, share, highest, total)


def put_blocks(payload, kept, first, entries, entry_at, size):
    for index in range(entries):
        payload[first + index * size : first + (index + 1) * size] = entry_at(0, index)
        kept[index * size : (index + 1) * size] = entry_at(1, index)


def merge_near_kernel(share, block_rows, groups, place_s, *refs):
    pieces, (payload, kept, sources) = refs[:-3], refs[-3:]
    near, far = place_s[0], place_s[1]
    first = share + small_count(share)
    smalls = [get_small(piece[share:first], share) for piece in pieces]
    highest = smalls[0][0]
    for maxima, _ in smalls[1:]:
        highest = jnp.maximum(highest, maxima)
    total, mixture = 0.0, 0.0
    for piece, (maxima, totals) in zip(pieces, smalls):
        factor = jnp.exp(maxima - highest)
        total += totals * factor
        mixture += piece[:share] * spread_rows(factor)
    put_state(payload, share, highest, total, mixture)
    for group in range(groups):
        for at, piece in enumerate(pieces):
            source = first + group * block_rows
            sources[group, pl.ds((near ^ at) * block_rows, block_rows)] = piece[source : source + block_rows]
    bit = far & 1

    def entry_at(mine, index):
        return sources[2 * index + (bit if mine else 1 - bit)]

    put_blocks(payload, kept, first, groups // 2, entry_at, sources.shape[1])


def far_merge(step, share, entry, place_s, own, kept, got, blocks):
    bit = (place_s[1] >> step) & 1
    first = share + small_count(share)
    entries = kept.shape[0] // entry
    width = 1 << step
    for index in range(entries):
        target, source = index // width, index % width
        at = target * 2 * width + source
        blocks[at + bit * width] = kept[index * entry : (index + 1) * entry]
        blocks[at + (1 - bit) * width] = got[first + index * entry : first + (index + 1) * entry]
    parts = []
    for rows, rows_other in ((own, got), (got, own)):
        pick = lambda at: jnp.where(bit == 0, rows[at], rows_other[at])
        maxima, totals = get_small(pick(slice(share, first)), share)
        parts.append((maxima, totals, pick(slice(0, share))))
    return parts


def merge_mid_kernel(step, share, entry, place_s, own, kept, got, payload, next_kept, blocks):
    (low_max, low_total, low_mix), (high_max, high_total, high_mix) = far_merge(
        step, share, entry, place_s, own, kept, got, blocks
    )
    highest = jnp.maximum(low_max, high_max)
    low, high = jnp.exp(low_max - highest), jnp.exp(high_max - highest)
    put_state(
        payload,
        share,
        highest,
        low_total * low + high_total * high,
        low_mix * spread_rows(low) + high_mix * spread_rows(high),
    )
    bit = (place_s[1] >> (step + 1)) & 1
    width = 2 << step

    def entry_at(mine, index):
        target, source = index // width, index % width
        return blocks[(2 * target + (bit if mine else 1 - bit)) * width + source]

    put_blocks(payload, next_kept, share + small_count(share), blocks.shape[0] // 2, entry_at, entry)


def merge_far_kernel(units, step, entry, place_s, parents_s, queries, branch, own, kept, got, out, out_blocks, blocks):
    near = place_s[0]
    unit_rows = queries.shape[2]
    share = units * unit_rows
    group_size = unit_rows // BEAMS
    states = far_merge(step, share, entry, place_s, own, kept, got, blocks)
    for index in range(blocks.shape[0]):
        out_blocks[index * entry : (index + 1) * entry] = blocks[index]
    beam_id = lax.broadcasted_iota(jnp.int32, (BEAMS, HEAD_SIZE), 0)
    own_scores, own_values = [], []
    for u in range(units):
        unit = near * units + u
        layer, head = unit // KEY_VALUE_HEADS, unit % KEY_VALUE_HEADS
        lanes = pl.ds(pl.multiple_of(head * HEAD_SIZE, HEAD_SIZE), HEAD_SIZE)
        keys, values = (branch[layer, kind, :, lanes].astype(jnp.float32) for kind in range(2))

        def chosen(rows):
            picked = [
                jnp.sum(jnp.where(beam_id == parents_s[beam], rows, 0.0), axis=0, keepdims=True)
                for beam in range(BEAMS)
            ]
            return jnp.concatenate([jnp.broadcast_to(row, (group_size, HEAD_SIZE)) for row in picked])

        own_scores.append(
            jnp.sum(queries[layer, head].astype(jnp.float32) * chosen(keys), axis=1, keepdims=True)
        )
        own_values.append(chosen(values))
    own_score = as_row(jnp.concatenate(own_scores)) / math.sqrt(HEAD_SIZE)
    highest = own_score
    for maxima, _, _ in states:
        highest = jnp.maximum(highest, maxima)
    factors = [jnp.exp(maxima - highest) for maxima, _, _ in states]
    own_factor = jnp.exp(own_score - highest)
    total = own_factor
    for (_, totals, _), factor in zip(states, factors):
        total += totals * factor
    mixture = jnp.concatenate(own_values) * spread_rows(own_factor / total)
    for (_, _, part), factor in zip(states, factors):
        mixture += part * spread_rows(factor / total)
    out[...] = mixture


def assemble_kernel(units, place_s, *refs):
    pieces, out = refs[:-1], refs[-1]
    unit_rows = pieces[0].shape[0] // units
    group_size = unit_rows // BEAMS
    for step, piece in enumerate(pieces):
        for u in range(units):
            unit = (place_s[0] ^ step) * units + u
            layer, head = unit // KEY_VALUE_HEADS, unit % KEY_VALUE_HEADS
            for query in range(group_size):
                at = pl.multiple_of((head * group_size + query) * HEAD_SIZE, HEAD_SIZE)
                out[layer, :, pl.ds(at, HEAD_SIZE)] = piece[pl.ds(u * unit_rows + query, BEAMS, stride=group_size)]


def partial_of(rows):
    return pltpu.VMEM((rows, HEAD_SIZE), jnp.float32)


def attend(place, queried, kv_pages, page_scales, valid_pages, blocks):
    page_count, scale_count = page_scales.shape
    groups, inner, block_rows, _ = blocks.shape
    units = LAYERS * KEY_VALUE_HEADS // inner
    share = units * queried.shape[2]
    return pl.pallas_call(
        lambda *refs: attend_kernel(units, *refs),
        in_specs=[SMEM, SMEM, VMEM, VMEM, VMEM, ANY],
        out_specs=(VMEM,) * inner,
        out_shape=(partial_of(share + small_count(share) + groups * block_rows),) * inner,
        scratch_shapes=[
            pltpu.VMEM((scale_count, page_count * PAGE), jnp.float32),
            pltpu.VMEM((inner * units, page_count, 2, PAGE, HEAD_SIZE), kv_pages.dtype),
            pltpu.SemaphoreType.DMA((inner * units,)),
        ],
        compiler_params=pltpu.CompilerParams(vmem_limit_bytes=12 * MIB),
        name="attend",
    )(place, valid_pages, queried, page_scales.T, blocks, in_hbm(kv_pages))


def far_shapes(share, entry, groups):
    return (
        partial_of(share + small_count(share) + groups // 2 * entry),
        partial_of(groups // 2 * entry),
    )


def merge_near(place, pieces, share, block_rows, groups):
    entry = len(pieces) * block_rows
    return pl.pallas_call(
        lambda *refs: merge_near_kernel(share, block_rows, groups, *refs),
        in_specs=[SMEM] + [VMEM] * len(pieces),
        out_specs=(VMEM, VMEM),
        out_shape=far_shapes(share, entry, groups),
        scratch_shapes=[pltpu.VMEM((groups, entry, HEAD_SIZE), jnp.float32)],
        compiler_params=pltpu.CompilerParams(vmem_limit_bytes=4 * MIB),
        name="merge_near",
    )(place, *map(in_vmem, pieces))


def merge_mid(place, step, own, kept, got, share, entry, groups):
    return pl.pallas_call(
        lambda *refs: merge_mid_kernel(step, share, entry, *refs),
        in_specs=[SMEM] + [VMEM] * 3,
        out_specs=(VMEM, VMEM),
        out_shape=far_shapes(share, entry, groups),
        scratch_shapes=[pltpu.VMEM((groups, entry, HEAD_SIZE), jnp.float32)],
        compiler_params=pltpu.CompilerParams(vmem_limit_bytes=4 * MIB),
        name="merge_mid",
    )(place, *map(in_vmem, (own, kept, got)))


def merge_far(place, step, parents, queried, branch_kv, own, kept, got, share, entry, groups):
    units = share // queried.shape[2]
    return pl.pallas_call(
        lambda *refs: merge_far_kernel(units, step, entry, *refs),
        in_specs=[SMEM, SMEM] + [VMEM] * 5,
        out_specs=(VMEM, VMEM),
        out_shape=(partial_of(share), partial_of(groups * entry)),
        scratch_shapes=[pltpu.VMEM((groups, entry, HEAD_SIZE), jnp.float32)],
        compiler_params=pltpu.CompilerParams(vmem_limit_bytes=4 * MIB),
        name="merge_far",
    )(place, parents, queried, branch_kv, *map(in_vmem, (own, kept, got)))


def assemble(place, pieces, units):
    return pl.pallas_call(
        lambda *refs: assemble_kernel(units, *refs),
        in_specs=[SMEM] + [VMEM] * len(pieces),
        out_specs=VMEM,
        out_shape=jax.ShapeDtypeStruct((LAYERS, BEAMS, HQ * HEAD_SIZE), jnp.float32),
        compiler_params=pltpu.CompilerParams(vmem_limit_bytes=4 * MIB),
        name="assemble",
    )(place, *map(in_vmem, pieces))


def bits_of(devices):
    masks, mask = [], 1
    while mask < devices:
        masks.append(mask)
        mask *= 2
    return masks


def swap(array, mask, devices):
    return lax.ppermute(array, "seq", [(i, i ^ mask) for i in range(devices)])


def exchange_pages(pages):
    return lax.all_to_all(pages, "seq", split_axis=0, concat_axis=0, tiled=True)


def on_device(queries, kv_pages, page_scales, page_owner, valid_pages, branch_kv, parents):
    devices = lax.axis_size("seq")
    page_count = kv_pages.shape[0]
    slot_count = max(2, (page_count + devices - 1) // devices)
    first_slots = max(1, int(slot_count * FIRST_PART))
    own_max = slot_count * min(devices, page_count)
    group_size = HQ // KEY_VALUE_HEADS
    rows = LAYERS * BEAMS * HQ
    send_first = pack_first(kv_pages, page_owner, valid_pages, devices, first_slots)
    send_rest, send_scales = pack_rest(kv_pages, page_scales, page_owner, valid_pages, devices, slot_count, first_slots)
    recv_first = exchange_pages(send_first)
    recv_rest = exchange_pages(send_rest)

    me = lax.axis_index("seq")
    masks = bits_of(devices)
    inner = 2 * masks[(len(masks) - 1) // 2]
    groups = devices // inner
    share = rows // inner
    place = jnp.stack([me % inner, me // inner]).astype(jnp.int32)
    block_size = slot_count * page_scales.shape[1]
    block_rows = -(-block_size // HEAD_SIZE)
    blocks = send_scales.reshape(devices, block_size)
    blocks = jnp.pad(blocks, ((0, 0), (0, block_rows * HEAD_SIZE - block_size)))
    blocks = blocks.reshape(groups, inner, block_rows, HEAD_SIZE)
    queried = queries.reshape(LAYERS, BEAMS, KEY_VALUE_HEADS, group_size, HEAD_SIZE).swapaxes(1, 2)
    queried = queried.reshape(LAYERS, KEY_VALUE_HEADS, BEAMS * group_size, HEAD_SIZE)
    pieces = attend(place, queried, kv_pages, page_scales, valid_pages, blocks)

    def spread(parts, masks):
        return [parts[0]] + [swap(part, mask, devices) for part, mask in zip(parts[1:], masks)]

    pieces = spread(pieces, range(1, inner))
    own, kept = merge_near(place, pieces, share, block_rows, groups)
    entry = inner * block_rows
    far_masks = [mask for mask in masks if mask >= inner]
    for step, mask in enumerate(far_masks):
        got = swap(own, mask, devices)
        if mask != far_masks[-1]:
            own, kept = merge_mid(place, step, own, kept, got, share, entry, groups)
    mine, blocks = merge_far(
        place, len(far_masks) - 1, parents, queried, branch_kv, own, kept, got, share, entry, groups
    )
    pieces = spread([mine] * inner, range(1, inner))
    attended = assemble(place, pieces, share // (BEAMS * group_size))
    blocks = blocks.reshape(devices, block_rows * HEAD_SIZE)[:, :block_size]
    recv_scales = blocks.reshape(devices * slot_count, page_scales.shape[1]).astype(page_scales.dtype)
    counts = jnp.sum((recv_scales[:, 0] > 0).astype(jnp.int32).reshape(devices, slot_count), axis=1)
    page_cache, cache_scales_t = unpack_first(recv_first, recv_scales, counts, own_max)
    page_cache = unpack_rest(recv_rest, counts, page_cache, first_slots)
    return (page_cache, cache_scales_t.T, attended)


def solution(mesh):
    return jax.shard_map(
        on_device,
        mesh=mesh,
        in_specs=(P(), P("seq", None, None, None), P("seq", None), P("seq"), P("seq"), P(), P()),
        out_specs=(P("seq", None, None, None), P("seq", None), P()),
        check_vma=False,
    )
```
